128 devices in a mesh: shard: 8 (over y, core), model: 16 (over z, x).
Axes of the slice: x: 4, y: 4, z: 4, core: 2. Of those that a mesh axis runs over, the one named last changes fastest.
Arguments:
- train_gate: float32 [4096, 12288], P('shard', 'model'), may hold values from -0.125 to 0.125
- slow_gate: float32 [4096, 12288], P('shard', 'model'), may hold values from -0.09375 to 0.09375
- train_up: float32 [4096, 12288], P('shard', 'model'), may hold values from -0.125 to 0.125
- slow_up: float32 [4096, 12288], P('shard', 'model'), may hold values from -0.09375 to 0.09375
- norm_train: float32 [4096], P(('shard', 'model')), may hold values from 0.25 to 1.75
- norm_step: float32 [4096], P(('shard', 'model')), may hold values from -0.3 to 0.3
Outputs:
- serve_gate: bfloat16 [4096, 12288], P(None, 'model')
- serve_up: bfloat16 [4096, 12288], P(None, 'model')
- factor_gate: float32 [12288], P('model')
- factor_up: float32 [12288], P('model')
- serve_norm: bfloat16 [4096], replicated
- fresh_gate: float32 [4096, 12288], P('shard', 'model')
- fresh_up: float32 [4096, 12288], P('shard', 'model')
The draws below stay inside these ranges and needn't reach their ends.
All inputs are finite; a program needn't handle non-finite values. Where the reference program divides by a largest or mean magnitude, that divisor is 1e-20 or more.
Results may differ from the reference program's by a relative error of at most 0.001.
Values may be sent and summed in bfloat16 or wider, within the bound.
No kernel may reach another device: no remote copies, remote signals or barrier semaphores. Data moves between devices by JAX's collectives and lax.ppermute only.
A program may use at most 128 MiB of HBM per device.

```python
import jax
import jax.numpy as jnp

D_MODEL = 4096
D_INNER = 12288


def spiked(result, key, source, target, shards_of, factor):
    owner, partner = [(jnp.arange(result.shape[position]) // (result.shape[position] // shards_of)).reshape([-1 if axis == position else 1 for axis in range(result.ndim)]) for position in (source, target)]
    chosen = jax.random.permutation(key, shards_of)[partner]
    strong = (owner == chosen) | (owner == (partner + shards_of // 2) % shards_of)
    return jnp.where(strong, factor * result, result)


def shard_levels(rng, shape, shards, smallest, high):
    def one(position, shards_of):
        steps = jax.random.uniform(jax.random.fold_in(jax.random.fold_in(rng, 6), position), (shards_of,), jnp.float32, smallest / len(shards), high / len(shards))
        return jnp.repeat(jnp.exp(steps), shape[position] // shards_of).reshape((-1,) + (1,) * (len(shape) - position - 1))

    loudness = one(*shards[0])
    for cut in shards[1:]:
        loudness = loudness * one(*cut)
    return loudness


def noise(rng, dims, width, reach, cuts=(), held_as=jnp.bfloat16):
    factor_of = shard_levels(rng, dims, cuts, -0.22, 0.18) if cuts else 1.0
    drawn = jax.random.normal(rng, dims, jnp.float32) * width * factor_of
    return jnp.minimum(jnp.maximum(drawn, -reach), reach).astype(held_as)


def noise_with(rng, shape, spread, most, shards, heavy, kind=jnp.bfloat16):
    array = spread * jax.random.normal(rng, shape, jnp.float32)
    if shards:
        array = array * shard_levels(rng, shape, shards, -0.22, 0.18)
    return jnp.clip(spiked(array, jax.random.fold_in(rng, 3), *heavy), -most, most).astype(kind)


def setup_inputs(seed: int = 0) -> dict:
    splits = jax.random.split(jax.random.key(seed), 7)
    train_gate = noise_with(splits[0], (D_MODEL, D_INNER), D_MODEL ** -0.5, 0.125, ((0, 8), (1, 16)), (0, 1, 16, 2.0), jnp.float32)
    slow_gate = noise(splits[1], (D_MODEL, D_INNER), D_MODEL ** -0.5, 0.09375, ((0, 8), (1, 16)), jnp.float32)
    train_up = noise_with(splits[2], (D_MODEL, D_INNER), D_MODEL ** -0.5, 0.125, ((0, 8), (1, 16)), (0, 1, 16, 2.0), jnp.float32)
    slow_up = noise(splits[3], (D_MODEL, D_INNER), D_MODEL ** -0.5, 0.09375, ((0, 8), (1, 16)), jnp.float32)
    norm_train = jnp.clip(1.0 + 0.15 * jax.random.normal(splits[4], (D_MODEL,), jnp.float32), 0.25, 1.75)
    norm_step = jnp.clip(jax.random.uniform(splits[5], (D_MODEL,), jnp.float32, -0.3, 0.3) * shard_levels(splits[5], (D_MODEL,), ((0, 128),), -0.4, 0.0), -0.3, 0.3)
    return dict(train_gate=train_gate, slow_gate=slow_gate, train_up=train_up, slow_up=slow_up, norm_train=norm_train, norm_step=norm_step)


keep_rate = 0.75


def reference(train_gate, slow_gate, train_up, slow_up, norm_train, norm_step):
    fresh_gate = keep_rate * slow_gate + (1.0 - keep_rate) * train_gate
    fresh_up = keep_rate * slow_up + (1.0 - keep_rate) * train_up
    factor_gate = jnp.sum(jnp.abs(fresh_gate), axis=0) / D_MODEL
    serve_gate = (fresh_gate / factor_gate).astype(jnp.bfloat16)
    factor_up = jnp.sum(jnp.abs(fresh_up), axis=0) / D_MODEL
    serve_up = (fresh_up / factor_up).astype(jnp.bfloat16)
    serve_norm = (norm_train + norm_step).astype(jnp.bfloat16)
    return serve_gate, serve_up, factor_gate, factor_up, serve_norm, fresh_gate, fresh_up
```

```python
import jax
import jax.numpy as jnp
from jax import lax
from jax.experimental import pallas as pl
from jax.experimental.pallas import tpu as pltpu
from jax.sharding import Mesh
from jax.sharding import PartitionSpec as P


D_MODEL = 4096
Y, CORE, Z, X = "y", "core", "z", "x"
keep_rate = 0.75
TINY = 1e-30


def shifted(array, axis, step):
    n = lax.axis_size(axis)
    return lax.ppermute(array, axis, [(i, (i + step) % n) for i in range(n)])


def swapped(array, axis, mask):
    return lax.ppermute(array, axis, [(i, i ^ mask) for i in range(lax.axis_size(axis))])


def onward(array):
    pairs = [(2 * y + c, 2 * ((y + (1, -1)[c]) % 4) + c) for y in range(4) for c in range(2)]
    return lax.ppermute(array, (Y, CORE), pairs)


def unwritten(shape):
    anywhere = pl.BlockSpec(memory_space=pl.ANY)
    return pl.pallas_call(
        lambda a, b: None,
        out_shape=(jax.ShapeDtypeStruct(shape, jnp.bfloat16),) * 2,
        out_specs=(anywhere, anywhere),
        compiler_params=pltpu.CompilerParams(vmem_limit_bytes=1 << 20),
    )()


def mixed(slow, train):
    return keep_rate * slow + (1.0 - keep_rate) * train


def coded(rows, sums):
    return (rows * (256.0 / jnp.maximum(sums, TINY))).astype(jnp.float16)


def decoded(code, sums, factor):
    scale = jnp.maximum(sums, TINY) * (1.0 / 256.0) / factor
    return (code.astype(jnp.float32) * scale).astype(jnp.bfloat16)


def body(train_gate, slow_gate, train_up, slow_up, norm_train, norm_step):
    y, c, z, x = (lax.axis_index(a) for a in (Y, CORE, Z, X))
    rows, cols = train_gate.shape

    fresh_gate, fresh_up = mixed(slow_gate, train_gate), mixed(slow_up, train_up)
    sg = jnp.sum(jnp.abs(fresh_gate), axis=0)
    su = jnp.sum(jnp.abs(fresh_up), axis=0)
    code_gate = coded(fresh_gate, sg)
    code_up = coded(fresh_up, su)
    eg = onward(code_gate)
    norm = (norm_train + norm_step).astype(jnp.bfloat16)
    slots = jnp.zeros((128 * norm.size,), jnp.float32)
    device = ((y * 2 + c) * 4 + z) * 4 + x
    slots = lax.dynamic_update_slice(slots, norm.astype(jnp.float32), (device * norm.size,))
    sums = jnp.concatenate([sg, su, slots])
    other = swapped(sums, CORE, 1)
    pfg, pfu = swapped(fresh_gate, CORE, 1), swapped(fresh_up, CORE, 1)
    pair = sums + other
    note = jnp.concatenate([pair, sg, su])
    far = shifted(pair, Y, 2)
    right, left = shifted(note, Y, 1), shifted(note, Y, -1)
    eu = onward(code_up)
    n = pair.size
    total = (pair + far) + (right[:n] + left[:n])
    factor_gate, factor_up = total[:cols] / D_MODEL, total[cols : 2 * cols] / D_MODEL
    behind = jnp.where(c == 0, right[n:], left[n:])

    gates, ups = unwritten((8 * rows, cols))
    back = jnp.where(c == 0, -1, 1)

    def put(out, block, dy, core):
        at = (((y + dy) & 3) * 2 + core) * rows
        return lax.dynamic_update_slice(out, block, (at, jnp.int32(0)))

    def normal(fresh, factor):
        return (fresh / factor).astype(jnp.bfloat16)

    block = normal(pfg, factor_gate)
    gates = put(gates, block, 0, c ^ 1)
    ng = onward(block)
    block = normal(pfu, factor_up)
    ups = put(ups, block, 0, c ^ 1)
    nu = onward(block)
    gates = put(gates, normal(fresh_gate, factor_gate), 0, c)
    ups = put(ups, normal(fresh_up, factor_up), 0, c)

    block = decoded(eg, behind[:cols], factor_gate)
    gates = put(gates, block, back, c)
    seg = swapped(block, CORE, 1)
    block = decoded(eu, behind[cols:], factor_up)
    ups = put(ups, block, back, c)
    seu = swapped(block, CORE, 1)
    gates = put(gates, seg, -back, c ^ 1)
    ups = put(ups, seu, -back, c ^ 1)

    slots = total[2 * cols :].astype(jnp.bfloat16)
    for axis, mask in ((X, 1), (X, 3), (Z, 1), (Z, 3)):
        slots = slots + swapped(slots, axis, mask)
    serve_norm = slots

    fg, fu = onward(ng), onward(nu)
    sng, snu = swapped(ng, CORE, 1), swapped(nu, CORE, 1)
    gates = put(gates, ng, back, c ^ 1)
    gates = put(gates, sng, -back, c)
    ups = put(ups, nu, back, c ^ 1)
    ups = put(ups, snu, -back, c)
    sfg, sfu = swapped(fg, CORE, 1), swapped(fu, CORE, 1)
    gates = put(gates, fg, 2, c ^ 1)
    gates = put(gates, sfg, 2, c)
    ups = put(ups, fu, 2, c ^ 1)
    ups = put(ups, sfu, 2, c)
    return (gates, ups, factor_gate, factor_up, serve_norm, fresh_gate, fresh_up)


def solution(mesh):
    split = Mesh(mesh.devices.reshape(4, 2, 4, 4), (Y, CORE, Z, X))
    weights = P((Y, CORE), (Z, X))
    columns = P((Z, X))
    every = P((Y, CORE, Z, X))
    return jax.shard_map(
        body,
        mesh=split,
        in_specs=(weights,) * 4 + (every,) * 2,
        out_specs=(P(None, (Z, X)), P(None, (Z, X)), columns, columns, P(), weights, weights),
        check_vma=False,
    )
```
